32 devices in a mesh: mats: 8 (over z, x), tp: 4 (over y, core).
Axes of the slice: x: 2, y: 2, z: 4, core: 2. Of those that a mesh axis runs over, the one named last changes fastest.
Arguments:
- grad: bfloat16 [3072, 16384], P('tp', 'mats'), may hold values from -40 to 40
- momentum: float32 [3072, 16384], P('tp', 'mats'), may hold values from -6 to 6
Outputs:
- update: bfloat16 [3072, 16384], P('tp', 'mats')
- new_momentum: float32 [3072, 16384], P('tp', 'mats')
The draws below stay inside these ranges and needn't reach their ends.
All inputs are finite; a program needn't handle non-finite values.
Results may differ from the reference program's by a relative error of at most 0.01.
Values may be sent and summed in bfloat16 or wider, within the bound.
A program may use at most 128 MiB of HBM per device.

```python
import math
import jax
import jax.numpy as jnp
from jax import lax

R = 3072
C = 16384
ITERS = 2


def draw_grad(key, part):
    keys = jax.random.split(jax.random.fold_in(key, 11), 3)
    position = jnp.arange(R, dtype=jnp.float32).reshape(R, 1) / (R - 1.0)
    rising = jnp.exp(math.log(0.1) * (1.0 - position))
    rough_rows = jax.random.uniform(keys[0], (R, 1), jnp.float32, 0.5, 1.0)
    row_scale = rising * rough_rows
    col_scale = jnp.exp(jax.random.uniform(keys[1], (1, C), jnp.float32, 0.0, math.log(10.0)))
    base = jax.random.normal(keys[2], (R, C), jnp.float32)
    base = jnp.clip(base, -4.0, 4.0)
    return (base * row_scale * col_scale).astype(jnp.bfloat16)


def level_of(own_key, extent, shards, low, largest):
    loudness = 1.0
    for dim, shards_of in shards:
        heights = jax.random.uniform(jax.random.fold_in(jax.random.fold_in(own_key, 6), dim), (shards_of,), jnp.float32, low / len(shards), largest / len(shards))
        loudness = loudness * jnp.repeat(jnp.exp(heights), extent[dim] // shards_of).reshape((-1,) + (1,) * (len(extent) - 1 - dim))
    return loudness


def normal_values(key, extent, width, reach, cuts=(), held_as=jnp.bfloat16):
    entries = width * jax.random.normal(key, extent, jnp.float32)
    if cuts:
        entries = entries * level_of(key, extent, cuts, -0.22, 0.18)
    return jnp.clip(entries, -reach, reach).astype(held_as)


def setup_inputs(seed: int = 0) -> dict:
    key_of = jax.random.split(jax.random.key(seed), 3)
    grad = draw_grad(jax.random.fold_in(key_of[2], 71), 0)
    momentum = normal_values(key_of[1], (R, C), 1.0, 6.0, ((0, 4), (1, 8)), jnp.float32)
    return {"grad": grad, "momentum": momentum}


momentum_beta = 0.95
first_coef = 3.4445
second_coef = -4.775
third_coef = 2.0315
shape_gain = 0.2
epsilon = 1e-06

def reference(grad, momentum):
    new_momentum = momentum_beta * momentum + grad.astype(jnp.float32)
    iterate = (grad.astype(jnp.float32) + momentum_beta * new_momentum).astype(jnp.bfloat16)
    for step in range(ITERS):
        gram = lax.dot_general(iterate, iterate, (((1,), (1,)), ((), ())), preferred_element_type=jnp.float32).astype(jnp.bfloat16)
        first = jnp.dot(gram, iterate, preferred_element_type=jnp.float32).astype(jnp.bfloat16)
        second = jnp.dot(gram, first, preferred_element_type=jnp.float32).astype(jnp.bfloat16)
        if step == 0:
            bound = jnp.max(lax.optimization_barrier(jnp.sum(jnp.abs(gram.astype(jnp.float32)), axis=1))) + epsilon
            root = lax.rsqrt(bound)
            mixed = first_coef * iterate.astype(jnp.float32) * root + second_coef * first.astype(jnp.float32) * root ** 3 + third_coef * second.astype(jnp.float32) * root ** 5
        else:
            mixed = first_coef * iterate.astype(jnp.float32) + second_coef * first.astype(jnp.float32) + third_coef * second.astype(jnp.float32)
        iterate = mixed.astype(jnp.bfloat16)
    update = (shape_gain * math.sqrt(max(R, C)) * iterate.astype(jnp.float32)).astype(jnp.bfloat16)
    return (update, new_momentum)
```

```python
import functools
import math

import jax
import jax.numpy as jnp
from jax import lax
from jax.experimental import pallas as pl
from jax.experimental.pallas import tpu as pltpu
from jax.sharding import PartitionSpec as P

momentum_beta = 0.95
first_coef = 3.4445
second_coef = -4.775
third_coef = 2.0315
shape_gain = 0.2
epsilon = 1e-06


def row_dot(left, right):
    return lax.dot_general(
        left, right, (((1,), (1,)), ((), ())), preferred_element_type=jnp.float32
    )


def chain_kernel(tile, scale, bound_ref, gram_ref, x_ref, out_ref, base, held, left, right, saved):
    rows = x_ref.shape[0]
    bound = bound_ref[0, 0]
    root = lax.rsqrt(jnp.full((1, x_ref.shape[1]), bound, jnp.float32))
    inverse = root * root

    def tiles(body):
        @pl.loop(0, rows // tile)
        def _(step):
            body(pl.ds(pl.multiple_of(step * tile, tile), tile))

    def product(at, source):
        return inverse * jnp.dot(
            gram_ref[at, :], source[...], preferred_element_type=jnp.float32
        )

    def apply(source, target):
        def body(at):
            target[at, :] = product(at, source).astype(jnp.bfloat16)

        tiles(body)

    def combine(at, zeroth, once, twice):
        return (
            first_coef * zeroth[at, :].astype(jnp.float32)
            + second_coef * once[at, :].astype(jnp.float32)
            + third_coef * twice
        )

    def polynomial(source, target):
        apply(source, left)

        def body(at):
            target[at, :] = combine(at, source, left, product(at, left)).astype(jnp.bfloat16)

        tiles(body)

    def normalize(at):
        right[at, :] = (x_ref[at, :].astype(jnp.float32) * root).astype(jnp.bfloat16)

    tiles(normalize)
    polynomial(right, base)

    def start(at):
        held[at, :] = base[at, :]

    tiles(start)

    @pl.loop(0, 2)
    def _(turn):
        polynomial(held, right)
        polynomial(right, right)
        apply(right, held)

        @pl.when(turn == 0)
        def _():
            def keep(at):
                saved[at, :] = held[at, :]

            tiles(keep)

    def finish(at):
        mixed = combine(at, base, saved, held[at, :].astype(jnp.float32)).astype(jnp.bfloat16)
        out_ref[at, :] = (scale * mixed.astype(jnp.float32)).astype(jnp.bfloat16)

    tiles(finish)


def per_device(scale, grad, momentum):
    new_momentum = momentum_beta * momentum + grad.astype(jnp.float32)
    iterate = (grad.astype(jnp.float32) + momentum_beta * new_momentum).astype(jnp.bfloat16)
    columns = lax.all_gather(iterate, "tp", axis=0, tiled=True)
    part = row_dot(iterate, columns).astype(jnp.bfloat16)
    share = lax.psum_scatter(part, "mats", scatter_dimension=0, tiled=True)
    peak = jnp.max(jnp.sum(jnp.abs(share.astype(jnp.float32)), axis=1))
    bound = lax.pmax(peak, ("tp", "mats")) + epsilon
    gram = lax.all_gather(share, ("tp", "mats"), axis=0, tiled=True)
    rows = columns.shape[0]
    width = columns.shape[1] // lax.axis_size("tp")
    own = lax.dynamic_slice_in_dim(columns, lax.axis_index("tp") * width, width, axis=1)
    tile = math.gcd(rows, 512)
    whole = pl.BlockSpec(memory_space=pltpu.VMEM)
    result = pl.pallas_call(
        functools.partial(chain_kernel, tile, scale),
        out_shape=jax.ShapeDtypeStruct(own.shape, jnp.bfloat16),
        in_specs=[pl.BlockSpec(memory_space=pltpu.SMEM), whole, whole],
        out_specs=whole,
        scratch_shapes=[pltpu.VMEM(own.shape, jnp.bfloat16)] * 5,
        compiler_params=pltpu.CompilerParams(vmem_limit_bytes=60 * 1024 * 1024),
        cost_estimate=pl.CostEstimate(
            flops=24 * rows * rows * width, bytes_accessed=2 * rows * rows, transcendentals=0
        ),
    )(bound.reshape(1, 1), gram, own)
    update = lax.all_to_all(result, "tp", 0, 1, tiled=True)
    return (update, new_momentum)


def solution(mesh):
    def step(grad, momentum):
        scale = shape_gain * math.sqrt(max(grad.shape))
        return jax.shard_map(
            functools.partial(per_device, scale),
            mesh=mesh,
            in_specs=(P("tp", "mats"), P("tp", "mats")),
            out_specs=(P("tp", "mats"), P("tp", "mats")),
            check_vma=False,
        )(grad, momentum)

    return step
```
